32 devices in a mesh: section: 4 (over y, x), seq: 8 (over z, core).
Axes of the slice: x: 2, y: 2, z: 4, core: 2. Of those that a mesh axis runs over, the one named last changes fastest.
Arguments:
- patches: bfloat16 [8, 729, 1152], P('seq'), may hold values from -40 to 40
- fc_gain: float32 [4, 1152], P('section'), may hold values from 0.1 to 1.9
- fc_in: bfloat16 [4, 1152, 2176], P('section', 'seq'), may hold values from -0.1875 to 0.1875
- fc_in_bias: float32 [4, 2176], P('section'), may hold values from -3 to 3
- fc_out: bfloat16 [4, 2176, 1152], P('section', None, 'seq'), may hold values from -0.125 to 0.125
- fc_out_bias: float32 [4, 1152], P('section'), may hold values from -3 to 3
- proj_weight: bfloat16 [1152, 3584], P('seq'), may hold values from -0.1875 to 0.1875
- text_embed: bfloat16 [1024, 3584], P('seq'), may hold values from -40 to 40
- frame_start: int32 [8], replicated, may hold values from 0 to 1023, as said below
- frame_count: int32 [8], replicated, may hold values from 1 to 196, as said below
- segment_ids: int32 [1024], replicated, may hold values from 0 to 2, as said below
- norm_gain: float32 [3584], replicated, may hold values from 0.1 to 1.9
- query_weight: bfloat16 [3584, 2048], P(None, 'section'), may hold values from -3 to 3
- query_bias: float32 [2048], P('section'), may hold values from -3 to 3
- key_weight: bfloat16 [3584, 512], P(None, 'section'), may hold values from -1 to 1
- value_weight: bfloat16 [3584, 512], P(None, 'section'), may hold values from -0.09375 to 0.09375
- value_bias: float32 [512], P('section'), may hold values from -3 to 3
Outputs:
- attended: bfloat16 [1024, 2048], P('seq', 'section')
The draws below stay inside these ranges and needn't reach their ends.
Inputs may be any that keep to these rules, and one draw needn't show every extreme that they name: Frame f keeps its first frame_count[f] pooled tokens and places them at positions frame_start[f] to frame_start[f] + frame_count[f] - 1; frame f begins in shard f, at a position from f * 128 to (f + 1) * 128 - 1; every frame ends before the next one begins, and the last ends by position 1023. The frame of shard 8 / 2 - 1 runs into the next shard. `frame_count`: some frame keeps all 196 tokens. `segment_ids`: segment numbers never fall along the sequence, and each of 0, 1 and 2 occurs.
All inputs are finite; a program needn't handle non-finite values.
Results may differ from the reference program's by a relative error of at most 0.02.
Values may be sent and summed in bfloat16 or wider, within the bound.
A program may use at most 128 MiB of HBM per device.

```python
import math
import jax
import jax.numpy as jnp
from jax import lax

D = 1152
FF = 2176
GRID = 27
HM = 3584
HEAD = 128
KV_HEADS = 4
QPK = 4
L_DEV = 128
PATCH = 729
POOLED = 196
QHEADS = 16
LAYERS = 4
FRAMES = 8
L_TOTAL = 1024
N_SEQ = 8


def rough_field(key, lead_shape, feature_width):
    k_base, k_rows, k_cols = jax.random.split(key, 3)
    base_draw = jax.random.normal(k_base, lead_shape + (feature_width,), jnp.float32)
    base_draw = jnp.clip(base_draw, -4.0, 4.0)
    row_scale = jnp.exp(jax.random.uniform(k_rows, lead_shape + (1,), jnp.float32, -1.15, 1.15))
    col_scale = jnp.exp(jax.random.uniform(k_cols, (feature_width,), jnp.float32, -1.15, 1.15))
    return base_draw * row_scale * col_scale


def draw_patches(key, part):
    return rough_field(jax.random.fold_in(key, 3), (FRAMES, PATCH), D).astype(jnp.bfloat16)


def draw_text_embed(key, part):
    return rough_field(jax.random.fold_in(key, 4), (L_TOTAL,), HM).astype(jnp.bfloat16)


def attention_pair(key):
    k_keys, k_noise = jax.random.split(jax.random.fold_in(key, 7), 2)
    root_width = math.sqrt(HM)
    key_draw = jnp.clip(jax.random.normal(k_keys, (HM, KV_HEADS, 1, HEAD), jnp.float32), -6.0, 6.0) / root_width
    noise_draw = jnp.clip(jax.random.normal(k_noise, (HM, KV_HEADS, QPK, HEAD), jnp.float32), -6.0, 6.0) * (3.5 / root_width)
    queries = noise_draw
    queries = jnp.clip(queries, -3.0, 3.0).reshape(HM, KV_HEADS * QPK * HEAD)
    return (key_draw.reshape(HM, KV_HEADS * HEAD), queries)


def draw_query_weight(key, part):
    return attention_pair(key)[1].astype(jnp.bfloat16)


def draw_key_weight(key, part):
    return attention_pair(key)[0].astype(jnp.bfloat16)


def frame_layout(key):
    k_offsets, k_chosen, k_counts = jax.random.split(jax.random.fold_in(key, 13), 3)
    middle = FRAMES // 2 - 1
    offsets = jax.random.randint(k_offsets, (FRAMES,), 0, L_DEV)
    chosen = jax.random.randint(k_chosen, (), 0, FRAMES - 4)
    chosen = jnp.where(chosen >= middle - 1, chosen + 3, chosen)
    frame_index = jnp.arange(FRAMES)
    offsets = jnp.where(frame_index == chosen, 0, offsets)
    offsets = jnp.where(frame_index == chosen + 1, max(POOLED - L_DEV, 0), offsets)
    offsets = jnp.where((frame_index == middle) | (frame_index == middle + 1), L_DEV - 1, offsets)
    following = jnp.concatenate([offsets[1:], jnp.zeros((1,), offsets.dtype)])
    upper_limit = jnp.minimum(POOLED, L_DEV + following - offsets)
    upper_limit = jnp.where(frame_index == FRAMES - 1, jnp.minimum(POOLED, L_DEV - offsets), upper_limit)
    lower_limit = jnp.maximum(1, upper_limit // 2)
    counts = jax.random.randint(k_counts, (FRAMES,), lower_limit, upper_limit + 1)
    counts = jnp.where(frame_index == chosen, POOLED, counts)
    counts = jnp.where(frame_index == middle, upper_limit, counts)
    starts = frame_index * L_DEV + offsets
    return (starts.astype(jnp.int32), counts.astype(jnp.int32))


def draw_frame_start(key, part):
    return frame_layout(key)[0]


def draw_frame_count(key, part):
    return frame_layout(key)[1]


def draw_segment_ids(key, part):
    k_first, k_second = jax.random.split(jax.random.fold_in(key, 5))
    first_cut = jax.random.randint(k_first, (), L_TOTAL // 16, L_TOTAL // 8)
    second_cut = jax.random.randint(k_second, (), L_TOTAL // 8, L_TOTAL // 4)
    positions = jnp.arange(L_TOTAL)
    return ((positions >= first_cut).astype(jnp.int32) + (positions >= second_cut).astype(jnp.int32)).astype(jnp.int32)


def block_levels(own_key, dims, cuts, least, largest):
    def one(position, parts):
        draws = jax.random.uniform(jax.random.fold_in(jax.random.fold_in(own_key, 6), position), (parts,), jnp.float32, least / len(cuts), largest / len(cuts))
        return jnp.repeat(jnp.exp(draws), dims[position] // parts).reshape((-1,) + (1,) * (len(dims) - position - 1))

    gain = one(*cuts[0])
    for cut in cuts[1:]:
        gain = gain * one(*cut)
    return gain


def noise(rng, dims, deviation, reach, pieces=(), kind=jnp.bfloat16):
    gain = block_levels(rng, dims, pieces, -0.22, 0.18) if pieces else 1.0
    array = jax.random.normal(rng, dims, jnp.float32) * deviation * gain
    return jnp.minimum(jnp.maximum(array, -reach), reach).astype(kind)


def setup_inputs(seed: int = 0) -> dict:
    arg_keys = jax.random.split(jax.random.key(seed), 18)
    patches = draw_patches(jax.random.fold_in(arg_keys[17], 71), 0)
    fc_gain = jnp.clip(1.0 + 0.18 * jax.random.normal(arg_keys[1], (LAYERS, D), jnp.float32), 0.1, 1.9)
    fc_in = noise(arg_keys[2], (LAYERS, D, FF), D ** -0.5, 0.1875, ((0, 4), (1, 8)))
    fc_in_bias = noise(arg_keys[3], (LAYERS, FF), 0.5, 3.0, ((0, 4),), jnp.float32)
    fc_out = noise(arg_keys[4], (LAYERS, FF, D), FF ** -0.5, 0.125, ((0, 4), (2, 8)))
    fc_out_bias = noise(arg_keys[5], (LAYERS, D), 0.5, 3.0, ((0, 4),), jnp.float32)
    proj_weight = noise(arg_keys[6], (D, HM), D ** -0.5, 0.1875, ((0, 8),))
    text_embed = draw_text_embed(jax.random.fold_in(arg_keys[17], 71), 0)
    frame_start = draw_frame_start(jax.random.fold_in(arg_keys[17], 71), 0)
    frame_count = draw_frame_count(jax.random.fold_in(arg_keys[17], 71), 0)
    segment_ids = draw_segment_ids(jax.random.fold_in(arg_keys[17], 71), 0)
    norm_gain = jnp.clip(1.0 + 0.18 * jax.random.normal(arg_keys[11], (HM,), jnp.float32), 0.1, 1.9)
    query_weight = draw_query_weight(jax.random.fold_in(arg_keys[17], 71), 0)
    query_bias = noise(arg_keys[13], (QHEADS * HEAD,), 0.5, 3.0, ((0, 4),), jnp.float32)
    key_weight = draw_key_weight(jax.random.fold_in(arg_keys[17], 71), 0)
    value_weight = noise(arg_keys[15], (HM, KV_HEADS * HEAD), HM ** -0.5, 0.09375, ((1, 4),))
    value_bias = noise(arg_keys[16], (KV_HEADS * HEAD,), 0.5, 3.0, ((0, 4),), jnp.float32)
    return {"patches": patches, "fc_gain": fc_gain, "fc_in": fc_in, "fc_in_bias": fc_in_bias, "fc_out": fc_out, "fc_out_bias": fc_out_bias, "proj_weight": proj_weight, "text_embed": text_embed, "frame_start": frame_start, "frame_count": frame_count, "segment_ids": segment_ids, "norm_gain": norm_gain, "query_weight": query_weight, "query_bias": query_bias, "key_weight": key_weight, "value_weight": value_weight, "value_bias": value_bias}


layer_eps = 1e-06
rms_eps = 1e-06
rope_base = 1000000.0

def layer_norm(values, scales):
    widened = values.astype(jnp.float32)
    center = widened - lax.optimization_barrier(jnp.mean(widened, axis=-1, keepdims=True))
    spread = lax.optimization_barrier(jnp.mean(center * center, axis=-1, keepdims=True))
    return center * lax.rsqrt(spread + layer_eps) * scales

def encoder_layer(values, scales, w_in, b_in, w_out, b_out):
    normed = layer_norm(values, scales).astype(jnp.bfloat16)
    hidden = jax.nn.gelu(jnp.dot(normed, w_in, preferred_element_type=jnp.float32) + b_in, approximate=True).astype(jnp.bfloat16)
    summed = values.astype(jnp.float32) + jnp.dot(hidden, w_out, preferred_element_type=jnp.float32) + b_out
    return summed.astype(jnp.bfloat16)

def pool_frame(encoded):
    lead_dims = encoded.shape[:-2]
    channel = encoded.shape[-1]
    grid_side = GRID
    pool_side = (GRID + 1) // 2
    grid_cells = encoded.astype(jnp.float32).reshape(lead_dims + (grid_side, grid_side, channel))
    pad_cells = 2 * pool_side - grid_side
    grid_cells = jnp.pad(grid_cells, [(0, 0)] * len(lead_dims) + [(0, pad_cells), (0, pad_cells), (0, 0)])
    totals = grid_cells.reshape(lead_dims + (pool_side, 2, pool_side, 2, channel)).sum(axis=(-4, -2))
    counts = jnp.minimum(2, grid_side - 2 * jnp.arange(pool_side)).astype(jnp.float32)
    cell_area = counts[:, None] * counts[None, :]
    return (totals / cell_area[..., None]).reshape(lead_dims + (pool_side * pool_side, channel))

def rotate(values, positions):
    head_dim = values.shape[-1]
    half_dim = head_dim // 2
    inv_rates = jnp.exp(jnp.arange(half_dim, dtype=jnp.float32) * (-2.0 * math.log(rope_base) / head_dim))
    angles = positions.astype(jnp.float32)[:, None] * inv_rates[None, :]
    cosine = jnp.cos(angles)[:, None, :]
    sine_part = jnp.sin(angles)[:, None, :]
    first_half = values[..., :half_dim]
    second = values[..., half_dim:]
    return jnp.concatenate([first_half * cosine - second * sine_part, second * cosine + first_half * sine_part], axis=-1)

def reference(patches, fc_gain, fc_in, fc_in_bias, fc_out, fc_out_bias, proj_weight, text_embed, frame_start, frame_count, segment_ids, norm_gain, query_weight, query_bias, key_weight, value_weight, value_bias):
    encoded = patches.reshape(FRAMES * PATCH, D)
    for layer_index in range(LAYERS):
        encoded = encoder_layer(encoded, fc_gain[layer_index], fc_in[layer_index], fc_in_bias[layer_index], fc_out[layer_index], fc_out_bias[layer_index])
    pooled = pool_frame(encoded.reshape(FRAMES, PATCH, D)).astype(jnp.bfloat16)
    projected = jnp.dot(pooled.reshape(FRAMES * POOLED, D), proj_weight, preferred_element_type=jnp.float32).astype(jnp.bfloat16)
    positions = jnp.arange(L_TOTAL, dtype=jnp.int32)
    home_frame = (positions // L_DEV).astype(jnp.int32)
    before = jnp.maximum(home_frame - 1, 0).astype(jnp.int32)

    def pick_tokens(frame_ids, ok_extra):
        offset = positions - frame_start[frame_ids]
        is_valid = ok_extra & (offset >= 0) & (offset < frame_count[frame_ids])
        picked = jnp.take(projected, frame_ids * POOLED + jnp.clip(offset, 0, POOLED - 1), axis=0)
        return (is_valid, picked)
    own_valid, own_rows = pick_tokens(home_frame, True)
    prev_valid, prev_rows = pick_tokens(before, home_frame > 0)
    inputs = jnp.where(own_valid[:, None], own_rows, jnp.where(prev_valid[:, None], prev_rows, text_embed))
    widened = inputs.astype(jnp.float32)
    normed = (widened * lax.rsqrt(lax.optimization_barrier(jnp.mean(widened * widened, axis=-1, keepdims=True)) + rms_eps) * norm_gain).astype(jnp.bfloat16)
    queries = jnp.dot(normed, query_weight, preferred_element_type=jnp.float32) + query_bias
    queries = rotate(queries.reshape(L_TOTAL, KV_HEADS * QPK, HEAD), positions).astype(jnp.bfloat16)
    key_heads = jnp.dot(normed, key_weight, preferred_element_type=jnp.float32)
    key_heads = rotate(key_heads.reshape(L_TOTAL, KV_HEADS, HEAD), positions).astype(jnp.bfloat16)
    values = (jnp.dot(normed, value_weight, preferred_element_type=jnp.float32) + value_bias).astype(jnp.bfloat16)
    values = values.reshape(L_TOTAL, KV_HEADS, HEAD)
    key_float = key_heads.astype(jnp.float32)
    value_float = values.astype(jnp.float32)
    score_scale = 1.0 / math.sqrt(HEAD)

    def attend_rows(block_index):
        row_start = (block_index * L_DEV).astype(jnp.int32)
        query_rows = lax.dynamic_slice_in_dim(queries, row_start, L_DEV, 0).astype(jnp.float32)
        query_rows = query_rows.reshape(L_DEV, KV_HEADS, QPK, HEAD)
        query_pos = row_start + jnp.arange(L_DEV, dtype=jnp.int32)
        query_seg = lax.dynamic_slice_in_dim(segment_ids, row_start, L_DEV, 0)
        scores = jnp.einsum('qgjd,kgd->gjqk', query_rows, key_float) * score_scale
        allowed = (positions[None, :] <= query_pos[:, None]) & (segment_ids[None, :] == query_seg[:, None])
        row_top = lax.optimization_barrier(jnp.max(jnp.where(allowed, scores, -jnp.inf), axis=-1, keepdims=True))
        weights = jnp.where(allowed, jnp.exp(scores - row_top), 0.0)
        row_total = lax.optimization_barrier(jnp.sum(weights, axis=-1))
        rounded = lax.optimization_barrier(weights.astype(jnp.bfloat16)).astype(jnp.float32)
        mixed = jnp.einsum('gjqk,kgd->qgjd', rounded, value_float)
        mixed = mixed / jnp.transpose(row_total, (2, 0, 1))[..., None]
        return mixed.reshape(L_DEV, KV_HEADS * QPK * HEAD).astype(jnp.bfloat16)
    attended = lax.map(attend_rows, jnp.arange(N_SEQ, dtype=jnp.int32))
    return attended.reshape(L_TOTAL, KV_HEADS * QPK * HEAD)
```

```python
import functools
import math

import jax
import jax.numpy as jnp
from jax import lax
from jax.experimental import pallas as pl
from jax.experimental.pallas import tpu as pltpu
from jax.sharding import PartitionSpec as P

GRID = 27


layer_eps = 1e-06
rms_eps = 1e-06
rope_base = 1000000.0
mask_floor = -1e30


def passed_along(block, axis, distance):
    devices = range(lax.axis_size(axis))
    route = [(i - distance, i) for i in devices if i - distance in devices]
    return lax.ppermute(block, axis, route)


def from_last(x, axis):
    last = lax.axis_size(axis) - 1
    total = x
    for other in range(last):
        total = total + lax.ppermute(x, axis, [(last, other)])
    return total


def layer_norm(values, scales):
    widened = values.astype(jnp.float32)
    center = widened - jnp.mean(widened, axis=-1, keepdims=True)
    spread = jnp.mean(center * center, axis=-1, keepdims=True)
    return center * lax.rsqrt(spread + layer_eps) * scales


def encoder_layer(values, scales, w_in, b_in, w_out, b_out):
    normed = layer_norm(values, scales).astype(jnp.bfloat16)
    hidden = jax.nn.gelu(
        jnp.dot(normed, w_in, preferred_element_type=jnp.float32) + b_in, approximate=True
    ).astype(jnp.bfloat16)
    summed = (
        values.astype(jnp.float32)
        + jnp.dot(hidden, w_out, preferred_element_type=jnp.float32)
        + b_out
    )
    return summed.astype(jnp.bfloat16)


MESH = pl.DeviceIdType.MESH


def greet(axis, targets):
    barrier = pltpu.get_barrier_semaphore()
    for target, present in targets:

        @pl.when(present)
        def _(target=target):
            pl.semaphore_signal(barrier, inc=1, device_id={axis: target}, device_id_type=MESH)

    peers = 0
    for _, present in targets:
        peers = peers + present.astype(jnp.int32)
    pl.semaphore_wait(barrier, peers)


def chain_kernel(count, *refs):
    srcs, outs = refs[:count], refs[count : 2 * count]
    up_s, up_r, dn_s, dn_r, pu_s, pu_r, pd_s, pd_r, own = refs[2 * count :]
    size = lax.axis_size("seq")
    chips = size // 2
    me = lax.axis_index("seq")
    chip, core = me // 2, me % 2
    partner = chip * 2 + 1 - core
    above = jnp.minimum(chip + 1, chips - 1) * 2 + core
    below = jnp.maximum(chip - 1, 0) * 2 + core
    has_up, has_down = chip < chips - 1, chip > 0

    def slot(m, j, c):
        rows = srcs[m].shape[0]
        return outs[m].at[pl.ds(pl.multiple_of((2 * j + c) * rows, rows), rows)]

    def copy(m, t, j, c, sems, target):
        return pltpu.make_async_remote_copy(
            src_ref=srcs[m] if t == 0 else slot(m, j, c),
            dst_ref=slot(m, j, c),
            send_sem=sems[0].at[t, m],
            recv_sem=sems[1].at[t, m],
            device_id={"seq": target},
            device_id_type=MESH,
        )

    up, down, pu, pd = (up_s, up_r), (dn_s, dn_r), (pu_s, pu_r), (pd_s, pd_r)
    greet("seq", [(above, has_up), (below, has_down), (partner, me >= 0)])
    for m in range(count):
        pltpu.make_async_copy(srcs[m], slot(m, chip, core), own.at[m]).start()
    for t in range(chips):
        for m in range(count):

            @pl.when(chip - t >= 0)
            def _(t=t, m=m):
                j = chip - t
                if t > 0:
                    copy(m, t - 1, j, core, up, above).wait_recv()

                @pl.when(has_up)
                def _():
                    copy(m, t, j, core, up, above).start()

                copy(m, t, j, core, pu, partner).start()

            @pl.when(chip + t < chips)
            def _(t=t, m=m):
                j = chip + t
                if t > 0:
                    copy(m, t - 1, j, core, down, below).wait_recv()

                @pl.when(has_down)
                def _():
                    copy(m, t, j, core, down, below).start()

                if t > 0:
                    copy(m, t, j, core, pd, partner).start()

    for m in range(count):
        pltpu.make_async_copy(srcs[m], slot(m, chip, core), own.at[m]).wait()
    for t in range(chips):
        for m in range(count):

            @pl.when(chip - t >= 0)
            def _(t=t, m=m):
                j = chip - t

                @pl.when(has_up)
                def _():
                    copy(m, t, j, core, up, above).wait_send()

                copy(m, t, j, core, pu, partner).wait_send()
                copy(m, t, j, 1 - core, pu, partner).wait_recv()

            @pl.when(chip + t < chips)
            def _(t=t, m=m):
                j = chip + t

                @pl.when(has_down)
                def _():
                    copy(m, t, j, core, down, below).wait_send()

                if t > 0:
                    copy(m, t, j, core, pd, partner).wait_send()
                    copy(m, t, j, 1 - core, pd, partner).wait_recv()


def chain_gather(blocks, call_id, where):
    size = lax.axis_size("seq")
    count = len(blocks)
    return pl.pallas_call(
        functools.partial(chain_kernel, count),
        out_shape=[
            jax.ShapeDtypeStruct((b.shape[0] * size, b.shape[1]), b.dtype) for b in blocks
        ],
        in_specs=[pl.BlockSpec(memory_space=pltpu.VMEM)] * count,
        out_specs=[pl.BlockSpec(memory_space=where)] * count,
        scratch_shapes=[pltpu.SemaphoreType.DMA((size // 2, count))] * 8
        + [pltpu.SemaphoreType.DMA((count,))],
        compiler_params=pltpu.CompilerParams(collective_id=call_id, has_side_effects=True),
    )(*blocks)


def encode_kernel(
    rows, patches, gain, w_in, b_in, w_out_t, b_out, out, inbox, send_sem, recv_sem
):
    section = lax.axis_index("section")
    sections = lax.axis_size("section")
    following = jnp.minimum(section + 1, sections - 1)
    batches = patches.shape[0] // rows
    first = section == 0
    not_first, not_last = section > 0, section < sections - 1
    greet("section", [(following, not_last), (jnp.maximum(section - 1, 0), not_first)])

    def copy(b):
        block = pl.ds(pl.multiple_of(b * rows, rows), rows)
        return pltpu.make_async_remote_copy(
            src_ref=out.at[block],
            dst_ref=inbox.at[block],
            send_sem=send_sem.at[b],
            recv_sem=recv_sem.at[b],
            device_id={"section": following},
            device_id_type=MESH,
        )

    def run(b, carry):
        block = pl.ds(pl.multiple_of(b * rows, rows), rows)

        @pl.when(first)
        def _():
            inbox[block, :] = patches[block, :]

        @pl.when(not_first)
        def _():
            copy(b).wait_recv()

        values = inbox[block, :]
        normed = layer_norm(values, gain[...]).astype(jnp.bfloat16)
        pre = jnp.dot(normed, w_in[...], preferred_element_type=jnp.float32) + b_in[...]
        hidden = jax.nn.gelu(pre, approximate=True).astype(jnp.bfloat16)
        mixed = lax.dot_general(
            hidden, w_out_t[...], (((1,), (1,)), ((), ())), preferred_element_type=jnp.float32
        )
        out[block, :] = (values.astype(jnp.float32) + mixed + b_out[...]).astype(jnp.bfloat16)

        @pl.when(not_last)
        def _():
            copy(b).start()

        return carry

    lax.fori_loop(0, batches, run, 0)

    @pl.when(not_last)
    def _():
        def drain(b, carry):
            copy(b).wait_send()
            return carry

        lax.fori_loop(0, batches, drain, 0)


def encode(patches, gain, w_in, b_in, w_out_t, b_out, rows, call_id):
    batches = patches.shape[0] // rows
    whole = pl.BlockSpec(memory_space=pltpu.VMEM)
    return pl.pallas_call(
        functools.partial(encode_kernel, rows),
        out_shape=jax.ShapeDtypeStruct(patches.shape, patches.dtype),
        in_specs=[whole] * 6,
        out_specs=whole,
        scratch_shapes=[
            pltpu.VMEM(patches.shape, patches.dtype),
            pltpu.SemaphoreType.DMA((batches,)),
            pltpu.SemaphoreType.DMA((batches,)),
        ],
        compiler_params=pltpu.CompilerParams(
            collective_id=call_id, has_side_effects=True, vmem_limit_bytes=48 * 1024 * 1024
        ),
    )(patches, gain[None], w_in, b_in[None], w_out_t, b_out[None])


def pool_rows(offsets, counts_kept, patch_rows):
    pool_side = (GRID + 1) // 2
    token_i = (offsets // pool_side)[:, None]
    token_j = (offsets % pool_side)[:, None]
    patch = jnp.arange(patch_rows, dtype=jnp.int32)[None, :]
    patch_i, patch_j = patch // GRID, patch % GRID
    kept = ((offsets >= 0) & (offsets < counts_kept))[:, None]
    inside = kept & (patch_i // 2 == token_i) & (patch_j // 2 == token_j) & (patch < GRID * GRID)
    high = jnp.minimum(2, GRID - 2 * token_i)
    wide = jnp.minimum(2, GRID - 2 * token_j)
    share = 1.0 / jnp.maximum(high * wide, 1).astype(jnp.float32)
    return jnp.where(inside, share, 0.0).astype(jnp.bfloat16)


def rotate(values, positions):
    head_dim = values.shape[-1]
    half_dim = head_dim // 2
    inv_rates = jnp.exp(
        jnp.arange(half_dim, dtype=jnp.float32) * (-2.0 * math.log(rope_base) / head_dim)
    )
    angles = positions.astype(jnp.float32)[:, None] * inv_rates[None, :]
    cosine = jnp.cos(angles)[:, None, :]
    sine_part = jnp.sin(angles)[:, None, :]
    first_half = values[..., :half_dim]
    second = values[..., half_dim:]
    return jnp.concatenate(
        [first_half * cosine - second * sine_part, second * cosine + first_half * sine_part],
        axis=-1,
    )


def tail_kernel(
    tokens, text_h, proj_h, wq_h, wk_h, wv_h, gain, q_bias, v_bias, turn, segs, starts, counts,
    out, text, proj, wq, wk, wv, held, queries, pairs, load_s, send_s, recv_s, pass_s, got_s,
):
    size = lax.axis_size("seq")
    chips = size // 2
    me = lax.axis_index("seq")
    chip, core = me // 2, me % 2
    partner = chip * 2 + 1 - core
    rows, hm = text_h.shape
    head = wk_h.shape[1]
    group = wq_h.shape[1] // head
    tile = math.gcd(hm, 512)
    tiles = hm // tile

    def part(t):
        return pltpu.make_async_copy(
            proj_h.at[:, pl.ds(t * tile, tile)], proj.at[:, pl.ds(t * tile, tile)], load_s.at[t]
        )

    others = [(text_h, text), (wq_h, wq), (wk_h, wk), (wv_h, wv)]
    loads = [
        pltpu.make_async_copy(a, b, load_s.at[tiles + i]) for i, (a, b) in enumerate(others)
    ]
    loads[0].start()
    for t in range(tiles):
        part(t).start()
    for load in loads[1:]:
        load.start()

    barrier = pltpu.get_barrier_semaphore()

    def hail(other, carry):
        @pl.when(other != chip)
        def _():
            pl.semaphore_signal(
                barrier, inc=1, device_id={"seq": other * 2 + core}, device_id_type=MESH
            )

        return carry

    lax.fori_loop(0, chips, hail, 0)
    pl.semaphore_signal(barrier, inc=1, device_id={"seq": partner}, device_id_type=MESH)

    slot = lax.broadcasted_iota(jnp.int32, (rows, 1), 0) + me * rows
    before = jnp.maximum(me - 1, 0)
    own = slot - starts[me]
    prev = slot - starts[before]
    valid = ((own >= 0) & (own < counts[me])) | (
        (me > 0) & (prev >= 0) & (prev < counts[before])
    )
    loads[0].wait()
    squares = jnp.zeros((rows, 1), jnp.float32)
    for t in range(tiles):
        cols = slice(t * tile, (t + 1) * tile)
        part(t).wait()
        vision = jnp.dot(tokens[...], proj[:, cols], preferred_element_type=jnp.float32)
        mixed = jnp.where(
            valid, vision.astype(jnp.bfloat16).astype(jnp.float32), text[:, cols].astype(jnp.float32)
        )
        squares = squares + jnp.sum(mixed * mixed, axis=1, keepdims=True)
        held[:, cols] = mixed.astype(jnp.bfloat16)
    scale = lax.rsqrt(squares / hm + rms_eps)
    for t in range(tiles):
        cols = slice(t * tile, (t + 1) * tile)
        held[:, cols] = (held[:, cols].astype(jnp.float32) * scale * gain[:, cols]).astype(
            jnp.bfloat16
        )
    for load in loads[1:]:
        load.wait()
    half = head // 2
    cosine, sine = turn[:, :head], turn[:, head:]

    def spun(u):
        return u * cosine + jnp.concatenate([u[:, half:], u[:, :half]], axis=1) * sine

    normed = held[...]
    mine = pl.ds(pl.multiple_of(me * rows, rows), rows)
    keys = jnp.dot(normed, wk[...], preferred_element_type=jnp.float32)
    pairs[mine, :head] = spun(keys).astype(jnp.bfloat16)
    values = jnp.dot(normed, wv[...], preferred_element_type=jnp.float32) + v_bias[...]
    pairs[mine, head:] = values.astype(jnp.bfloat16)

    pl.semaphore_wait(barrier, chips)

    def above(other):
        return pltpu.make_async_remote_copy(
            src_ref=pairs.at[mine],
            dst_ref=pairs.at[mine],
            send_sem=send_s.at[other],
            recv_sem=recv_s.at[chip],
            device_id={"seq": other * 2 + core},
            device_id_type=MESH,
        )

    def across(source):
        block = pl.ds(pl.multiple_of((source * 2 + core) * rows, rows), rows)
        return pltpu.make_async_remote_copy(
            src_ref=pairs.at[block],
            dst_ref=pairs.at[block],
            send_sem=pass_s.at[source],
            recv_sem=got_s.at[source],
            device_id={"seq": partner},
            device_id_type=MESH,
        )

    def arriving(source, core_of, send, recv, target):
        block = pl.ds(pl.multiple_of((source * 2 + core_of) * rows, rows), rows)
        return pltpu.make_async_remote_copy(
            src_ref=pairs.at[block],
            dst_ref=pairs.at[block],
            send_sem=send.at[source],
            recv_sem=recv.at[source],
            device_id={"seq": target},
            device_id_type=MESH,
        )

    across(chip).start()

    def push(other, carry):
        above(other).start()
        return carry

    lax.fori_loop(chip + 1, chips, push, 0)
    asked = jnp.dot(normed, wq[...], preferred_element_type=jnp.float32) + q_bias[...]
    for h in range(group):
        queries[h * rows : (h + 1) * rows, :] = spun(asked[:, h * head : (h + 1) * head]).astype(
            jnp.bfloat16
        )

    def relay(i, carry):
        source = chip - 1 - i
        arriving(source, core, send_s, recv_s, partner).wait_recv()
        across(source).start()
        return carry

    lax.fori_loop(0, chip, relay, 0)

    def widened(j):
        row = segs[pl.ds(j, 1), :].astype(jnp.float32)
        return jnp.broadcast_to(row, (rows, rows))

    seg_q = widened(me).T
    seg_q = jnp.concatenate([seg_q, seg_q], axis=1)
    row_i = lax.broadcasted_iota(jnp.int32, (rows, 2 * rows), 0) + me * rows
    col_i = lax.broadcasted_iota(jnp.int32, (rows, 2 * rows), 1)
    spread = 1.0 / math.sqrt(head)

    def attend(i, carry):
        top, total, acc = carry
        source = chip - i
        arriving(source, 1 - core, pass_s, got_s, partner).wait_recv()
        block = pl.ds(pl.multiple_of(source * 2 * rows, 2 * rows), 2 * rows)
        seg_k = jnp.concatenate([widened(source * 2), widened(source * 2 + 1)], axis=1)
        allowed = (col_i + source * 2 * rows <= row_i) & (seg_k == seg_q)
        allowed = jnp.concatenate([jnp.where(allowed, 1.0, 0.0)] * group, axis=0) > 0.5
        score = (
            lax.dot_general(
                queries[...],
                pairs[block, :head],
                (((1,), (1,)), ((), ())),
                preferred_element_type=jnp.float32,
            )
            * spread
        )
        score = jnp.where(allowed, score, mask_floor)
        best = jnp.maximum(top, jnp.max(score, axis=1, keepdims=True))
        weight = jnp.where(allowed, jnp.exp(score - best), 0.0)
        fade = jnp.exp(top - best)
        total = total * fade + jnp.sum(weight, axis=1, keepdims=True)
        acc = acc * fade + jnp.dot(
            weight.astype(jnp.bfloat16), pairs[block, head:], preferred_element_type=jnp.float32
        )
        return best, total, acc

    start = (
        jnp.full((group * rows, 1), mask_floor, jnp.float32),
        jnp.zeros((group * rows, 1), jnp.float32),
        jnp.zeros((group * rows, head), jnp.float32),
    )
    _, total, acc = lax.fori_loop(0, chip + 1, attend, start)
    result = (acc / total).astype(jnp.bfloat16)
    for h in range(group):
        out[:, h * head : (h + 1) * head] = result[h * rows : (h + 1) * rows, :]

    def drain_push(other, carry):
        above(other).wait_send()
        return carry

    lax.fori_loop(chip + 1, chips, drain_push, 0)

    def drain_pass(source, carry):
        across(source).wait_send()
        return carry

    lax.fori_loop(0, chip + 1, drain_pass, 0)


def tail(tokens, text, proj, wq, wk, wv, gain, q_bias, v_bias, segment_ids, starts, counts, call_id):
    size = lax.axis_size("seq")
    chips = size // 2
    rows, hm = text.shape
    head = wk.shape[1]
    group = wq.shape[1] // head
    half = head // 2
    positions = lax.axis_index("seq") * rows + jnp.arange(rows, dtype=jnp.int32)
    rates = jnp.exp(
        jnp.arange(half, dtype=jnp.float32) * (-2.0 * math.log(rope_base) / head)
    )
    angles = positions.astype(jnp.float32)[:, None] * rates[None, :]
    c, s = jnp.cos(angles), jnp.sin(angles)
    turn = jnp.concatenate([c, c, -s, s], axis=1)
    tiles = hm // math.gcd(hm, 512)
    whole = pl.BlockSpec(memory_space=pltpu.VMEM)
    far = pl.BlockSpec(memory_space=pl.ANY)
    small = pl.BlockSpec(memory_space=pltpu.SMEM)
    dma = pltpu.SemaphoreType.DMA
    return pl.pallas_call(
        tail_kernel,
        out_shape=jax.ShapeDtypeStruct((rows, group * head), jnp.bfloat16),
        in_specs=[whole] + [far] * 5 + [whole] * 5 + [small] * 2,
        out_specs=whole,
        scratch_shapes=[
            pltpu.VMEM(text.shape, text.dtype),
            pltpu.VMEM(proj.shape, proj.dtype),
            pltpu.VMEM(wq.shape, wq.dtype),
            pltpu.VMEM(wk.shape, wk.dtype),
            pltpu.VMEM(wv.shape, wv.dtype),
            pltpu.VMEM((rows, hm), jnp.bfloat16),
            pltpu.VMEM((group * rows, head), jnp.bfloat16),
            pltpu.VMEM((size * rows, 2 * head), jnp.bfloat16),
            dma((tiles + 4,)),
            dma((chips,)),
            dma((chips,)),
            dma((chips,)),
            dma((chips,)),
        ],
        compiler_params=pltpu.CompilerParams(
            collective_id=call_id, has_side_effects=True, vmem_limit_bytes=48 * 1024 * 1024
        ),
    )(
        tokens, text, proj, wq, wk, wv, gain[None], q_bias[None], v_bias[None], turn,
        segment_ids.reshape(size, rows), starts, counts,
    )


def per_device(
    patches,
    fc_gain,
    fc_in,
    fc_in_bias,
    fc_out,
    fc_out_bias,
    proj_weight,
    text_embed,
    frame_start,
    frame_count,
    segment_ids,
    norm_gain,
    query_weight,
    query_bias,
    key_weight,
    value_weight,
    value_bias,
):
    section_count = lax.axis_size("section")
    section_id = lax.axis_index("section")
    shard_id = lax.axis_index("seq")
    shard_rows = text_embed.shape[0]
    head_size = key_weight.shape[1]
    group_size = query_weight.shape[1] // head_size
    frame_patches = patches[0]
    patch_rows, feature_width = frame_patches.shape
    aligned = fc_in.shape[1] % 16 == 0 and lax.axis_size("seq") % 2 == 0
    if aligned:
        w_in, w_out_t = chain_gather((fc_in[0], fc_out[0].T), 0, pl.ANY)
        proj_weight, w_in, w_out_t = lax.optimization_barrier((proj_weight, w_in, w_out_t))
    else:
        w_in = lax.all_gather(fc_in, "seq", axis=1, tiled=True)[0]
        w_out = lax.all_gather(fc_out, "seq", axis=2, tiled=True)[0]
    proj_full = lax.all_gather(proj_weight, "seq", axis=0, tiled=True)
    layer_gain = fc_gain[0]
    bias_in = fc_in_bias[0]
    bias_out = fc_out_bias[0]
    batch_rows = 96 if aligned else 128
    batches = -(-patch_rows // batch_rows)
    padded_rows = batches * batch_rows
    frame_patches = jnp.pad(frame_patches, [(0, padded_rows - patch_rows), (0, 0)])
    first_section = section_id == 0
    last_section = section_id == section_count - 1
    if aligned:
        collected = encode(
            frame_patches, layer_gain, w_in, bias_in, w_out_t, bias_out, batch_rows, 1
        )
    else:
        results = []
        for tick in range(batches + 2 * (section_count - 1)):
            start = min(tick, batches - 1) * batch_rows
            block = frame_patches[start : start + batch_rows]
            if tick >= 2:
                inflow = passed_along(results[tick - 2], "section", 1)
                block = jnp.where(first_section, block, inflow)
            results.append(encoder_layer(block, layer_gain, w_in, bias_in, w_out, bias_out))
        collected = jnp.concatenate(results[2 * (section_count - 1) :], axis=0)
    local_slots = jnp.arange(shard_rows, dtype=jnp.int32)
    positions = shard_id * shard_rows + local_slots
    own_start = frame_start[shard_id]
    own_count = frame_count[shard_id]
    previous = jnp.maximum(shard_id - 1, 0)
    own_offsets = positions - own_start
    own_valid = (own_offsets >= 0) & (own_offsets < own_count)
    prev_offsets = positions - frame_start[previous]
    prev_valid = (shard_id > 0) & (prev_offsets >= 0) & (prev_offsets < frame_count[previous])
    wanted = jnp.concatenate([own_offsets, own_offsets + shard_rows])
    pooled = jnp.dot(
        pool_rows(wanted, own_count, padded_rows), collected, preferred_element_type=jnp.float32
    ).astype(jnp.bfloat16)
    arrived = passed_along(pooled[shard_rows:], "seq", 1)
    tokens = jnp.where(own_valid[:, None], pooled[:shard_rows], arrived)
    tokens = jnp.where(last_section, tokens, jnp.zeros_like(tokens))
    tokens = from_last(tokens, "section")
    if aligned:
        return tail(
            tokens, text_embed, proj_full, query_weight, key_weight, value_weight, norm_gain,
            query_bias, value_bias, segment_ids, frame_start, frame_count, 2,
        )
    vision = jnp.dot(tokens, proj_full, preferred_element_type=jnp.float32).astype(jnp.bfloat16)
    inputs = jnp.where((own_valid | prev_valid)[:, None], vision, text_embed)
    widened = inputs.astype(jnp.float32)
    normed = (
        widened
        * lax.rsqrt(jnp.mean(widened * widened, axis=1, keepdims=True) + rms_eps)
        * norm_gain
    ).astype(jnp.bfloat16)
    queries = jnp.dot(normed, query_weight, preferred_element_type=jnp.float32) + query_bias
    queries = rotate(queries.reshape(shard_rows, group_size, head_size), positions).astype(
        jnp.bfloat16
    )
    queries = queries.reshape(shard_rows * group_size, head_size)
    key_heads = jnp.dot(normed, key_weight, preferred_element_type=jnp.float32)
    key_heads = rotate(key_heads.reshape(shard_rows, 1, head_size), positions).astype(jnp.bfloat16)
    key_heads = key_heads.reshape(shard_rows, head_size)
    values = (
        jnp.dot(normed, value_weight, preferred_element_type=jnp.float32) + value_bias
    ).astype(jnp.bfloat16)
    stacked = jnp.concatenate([key_heads, values], axis=1)
    query_pos = jnp.repeat(positions, group_size)
    query_seg = jnp.repeat(
        lax.dynamic_slice_in_dim(segment_ids, shard_id * shard_rows, shard_rows, 0), group_size
    )
    if aligned:
        (arrived_rows,) = chain_gather((stacked,), 2, pltpu.VMEM)
    else:
        arrived_rows = lax.all_gather(stacked, "seq", axis=0, tiled=True)
    key_part = arrived_rows[:, :head_size]
    value_part = arrived_rows[:, head_size:]
    scores = lax.dot_general(
        queries, key_part, (((1,), (1,)), ((), ())), preferred_element_type=jnp.float32
    ) * (1.0 / math.sqrt(head_size))
    key_pos = jnp.arange(arrived_rows.shape[0], dtype=jnp.int32)
    allowed = (key_pos[None, :] <= query_pos[:, None]) & (
        segment_ids[None, :] == query_seg[:, None]
    )
    masked = jnp.where(allowed, scores, mask_floor)
    weights = jnp.where(allowed, jnp.exp(masked - jnp.max(masked, axis=1, keepdims=True)), 0.0)
    row_total = jnp.sum(weights, axis=1, keepdims=True)
    row_acc = jnp.dot(
        weights.astype(jnp.bfloat16), value_part, preferred_element_type=jnp.float32
    )
    attended = (row_acc / row_total).astype(jnp.bfloat16)
    return attended.reshape(shard_rows, group_size * head_size)


def solution(mesh):
    return jax.shard_map(
        per_device,
        mesh=mesh,
        in_specs=(
            P("seq", None, None),
            P("section", None),
            P("section", "seq", None),
            P("section", None),
            P("section", None, "seq"),
            P("section", None),
            P("seq", None),
            P("seq", None),
            P(),
            P(),
            P(),
            P(),
            P(None, "section"),
            P("section"),
            P(None, "section"),
            P(None, "section"),
            P("section"),
        ),
        out_specs=P("seq", "section"),
        check_vma=False,
    )
```
